32 devices in a mesh: pair: 8 (over z, x), sector: 4 (over y, core).
Axes of the slice: x: 2, y: 2, z: 4, core: 2. Of those that a mesh axis runs over, the one named last changes fastest.
Arguments:
- wave: bfloat16 [4, 1024, 1024], P('sector', 'pair'), may hold values from -6 to 6
- left_ops: bfloat16 [16, 4, 1024, 1024], P('pair', 'sector'), may hold values from -0.1875 to 0.1875
- right_ops: bfloat16 [16, 4, 1024, 1024], P('pair', 'sector'), may hold values from -0.046875 to 0.046875
- targets: int32 [16, 4], P('pair', 'sector'), may hold values from -1 to 3
- sector_sizes: int32 [4], replicated, may hold values from 256 to 1024
- pair_ids: int32 [16], P('pair'), may hold values from 0 to 15, each once
- pair_coefficients: float32 [16], replicated, may hold values from 0.25 to 2
Outputs:
- sigma_blocks: float32 [4, 1024, 1024], P('sector', 'pair')
The draws below stay inside these ranges and needn't reach their ends.
Inputs may be any that keep to these rules, and one draw needn't show every extreme that they name: `pair_ids`: each orbital pair once.
All inputs are finite; a program needn't handle non-finite values.
Results may differ from the reference program's by a relative error of at most 0.0029.
Values may be sent and summed in bfloat16 or wider, within the bound.
No kernel may reach another device: no remote copies, remote signals or barrier semaphores. Data moves between devices by JAX's collectives and lax.ppermute only.
A program may use at most 128 MiB of HBM per device.

```python
import math
import jax
import jax.numpy as jnp
from jax import lax

BLOCK = 1024
SECTORS = 4
PAIRS = 16


def set_ends(values, own_key, low, largest):
    longest = values.shape.index(max(values.shape))
    spots = []
    for shift in (0, 1):
        where = [jax.random.randint(jax.random.fold_in(own_key, axis), (), 0, length) for axis, length in enumerate(values.shape)]
        where[longest] = (where[longest] + shift) % values.shape[longest]
        spots.append(tuple(where))
    return values.at[spots[0]].set(low).at[spots[1]].set(largest)


def levels(key, dims, cuts, low, top_value):
    gain = 1.0
    for axis_at, parts in cuts:
        heights = jax.random.uniform(jax.random.fold_in(jax.random.fold_in(key, 6), axis_at), (parts,), jnp.float32, low / len(cuts), top_value / len(cuts))
        gain = gain * jnp.repeat(jnp.exp(heights), dims[axis_at] // parts).reshape((-1,) + (1,) * (len(dims) - 1 - axis_at))
    return gain


def normal_values(rng, shape, deviation, reach, shards=(), held_as=jnp.bfloat16):
    level = levels(rng, shape, shards, -0.22, 0.18) if shards else 1.0
    values = jax.random.normal(rng, shape, jnp.float32) * deviation * level
    return jnp.minimum(jnp.maximum(values, -reach), reach).astype(held_as)


def setup_inputs(seed: int = 0) -> dict:
    arg_keys = jax.random.split(jax.random.key(seed), 8)
    return {
        "wave": normal_values(arg_keys[0], (SECTORS, BLOCK, BLOCK), 1.0, 6.0, ((0, 4), (1, 8))),
        "left_ops": normal_values(arg_keys[1], (PAIRS, SECTORS, BLOCK, BLOCK), BLOCK ** -0.5, 0.1875, ((0, 8), (1, 4))),
        "right_ops": normal_values(arg_keys[2], (PAIRS, SECTORS, BLOCK, BLOCK), (BLOCK * PAIRS) ** -0.5, 0.046875, ((0, 8), (1, 4))),
        "targets": set_ends(jax.random.randint(arg_keys[3], (PAIRS, SECTORS), -1, SECTORS), jax.random.fold_in(arg_keys[3], 1), -1, SECTORS - 1).astype(jnp.int32),
        "sector_sizes": set_ends(jax.random.randint(arg_keys[4], (SECTORS,), BLOCK // 4, BLOCK + 1), jax.random.fold_in(arg_keys[4], 1), BLOCK // 4, BLOCK).astype(jnp.int32),
        "pair_ids": jax.random.permutation(arg_keys[5], PAIRS).astype(jnp.int32),
        "pair_coefficients": jnp.clip(jnp.exp(jax.random.uniform(arg_keys[6], (PAIRS,), jnp.float32, math.log(0.25), math.log(2.0))), 0.25, 2.0),
    }


def reference(wave, left_ops, right_ops, targets, sector_sizes, pair_ids, pair_coefficients):
    positions = jnp.arange(BLOCK, dtype=jnp.int32)
    used = (positions[None, :] < sector_sizes[:, None]).astype(wave.dtype)
    masked = wave * used[:, :, None] * used[:, None, :]
    factor = pair_coefficients[pair_ids]
    sector_ids = jnp.arange(SECTORS, dtype=jnp.int32)

    def one_pair(totals, packed):
        left_op, right_op, target, weight = packed
        for source in range(SECTORS):
            left = jnp.dot(left_op[source], masked[source], preferred_element_type=jnp.float32).astype(jnp.bfloat16)
            term = lax.dot_general(left, right_op[source], (((1,), (1,)), ((), ())), preferred_element_type=jnp.float32)
            chosen = (sector_ids == target[source]).astype(jnp.float32)
            totals = totals + chosen[:, None, None] * (weight * term)[None]
        return totals, None

    start_totals = jnp.zeros((SECTORS, BLOCK, BLOCK), jnp.float32)
    totals, _ = lax.scan(one_pair, start_totals, (left_ops, right_ops, targets, factor))
    used_float = used.astype(jnp.float32)
    return totals * used_float[:, :, None] * used_float[:, None, :]
```

```python
import jax
import jax.numpy as jnp
from jax import lax
from jax.sharding import PartitionSpec as P

AXES = ("pair", "sector")
F32 = jnp.float32
BF16 = jnp.bfloat16


def route(pairs, sectors, move, allowed=lambda z, x, y, c: True):
    links = []
    for p in range(pairs):
        for s in range(sectors):
            spot = (p // 2, p % 2, s // 2, s % 2)
            if not allowed(*spot):
                continue
            z, x, y, c = move(*spot)
            if 0 <= z < pairs // 2:
                links.append((p * sectors + s, (z * 2 + x) * sectors + y * 2 + c))
    return links


def body(wave, left_ops, right_ops, targets, sector_sizes, pair_ids, pair_coefficients):
    block = wave.shape[2]
    rows = wave.shape[1]
    slots = left_ops.shape[0]
    pairs = lax.axis_size("pair")
    sectors = lax.axis_size("sector")
    depth = pairs // 2
    half = block // 2
    quarter = block // 4
    own_pair = lax.axis_index("pair")
    own_sector = lax.axis_index("sector")
    z, x = own_pair // 2, own_pair % 2
    y, c = own_sector // 2, own_sector % 2

    def send(value, move, allowed=lambda z, x, y, c: True):
        return lax.ppermute(value, AXES, route(pairs, sectors, move, allowed))

    def over_core(z, x, y, c):
        return z, x, y, 1 - c

    def over_x(z, x, y, c):
        return z, 1 - x, y, c

    def over_y(z, x, y, c):
        return z, x, 1 - y, c

    own_size = jnp.sum(jnp.where(jnp.arange(sectors) == own_sector, sector_sizes, 0))
    ids = jnp.arange(block, dtype=jnp.int32)
    used = ids < own_size
    row_used = own_pair * rows + jnp.arange(rows, dtype=jnp.int32) < own_size

    table_ids = jnp.arange(pair_coefficients.shape[0], dtype=jnp.int32)
    factor = jnp.sum(
        jnp.where(pair_ids[:, None] == table_ids[None, :], pair_coefficients[None, :], 0.0), axis=1
    )
    own_targets = targets[:, 0]
    other_targets = send(own_targets, over_core)

    own = wave[0]
    if depth <= 4:
        ups, downs = [], []
        up = down = own
        pieces = [(own, send(own, over_x))]
        for step in range(1, depth):
            up = send(up, lambda z, x, y, c: (z + 1, x, y, c), lambda z, x, y, c: z + 1 >= step)
            down = send(
                down, lambda z, x, y, c: (z - 1, x, y, c), lambda z, x, y, c: z - 1 < depth - step
            )
            ups.append((up, send(up, over_x, lambda z, x, y, c: z >= step)))
            downs.append((down, send(down, over_x, lambda z, x, y, c: z < depth - step)))
        chain = ups[::-1] + pieces + downs
        line = []
        for mine, theirs in chain:
            line.append(jnp.where(x == 0, mine, theirs))
            line.append(jnp.where(x == 0, theirs, mine))
        line = jnp.concatenate(line, axis=0)
        gathered = lax.dynamic_slice_in_dim(line, (depth - 1 - z) * 2 * rows, block, axis=0)
    else:
        gathered = lax.all_gather(own, "pair", axis=0, tiled=True)
    masked = gathered * (used[:, None] & used[None, :]).astype(gathered.dtype)

    left_mats = left_ops[:, 0].reshape(slots * block, block)
    left = jnp.dot(left_mats, masked, preferred_element_type=F32).astype(BF16)
    left = left.reshape(slots, block, block)

    def terms_of(core):
        mats = lax.dynamic_slice_in_dim(right_ops[:, 0], core * half, half, axis=1)
        term = lax.dot_general(
            left, mats, (((2,), (2,)), ((0,), (0,))), preferred_element_type=F32
        )
        return term * factor[:, None, None]

    given = terms_of(1 - c).astype(BF16)
    taken = send(given, over_core)
    kept = terms_of(c)

    def total(target, first):
        result = jnp.zeros((block, quarter), F32)
        for terms, aims in ((kept, own_targets), (taken, other_targets)):
            for slot in range(slots):
                part = terms[slot, :, first : first + quarter].astype(F32)
                result = result + jnp.where(aims[slot] == target, part, 0.0)
        return result.reshape(depth, 2, rows, quarter)

    def of_x(value, side):
        return jnp.where(side == 0, value[..., 0, :, :], value[..., 1, :, :])

    sent = jnp.stack([total(2 * (1 - y) + k, 0) for k in range(2)]).astype(BF16)
    first_y = send(sent, over_y)
    sent = jnp.stack([of_x(total(t, quarter), 1 - x) for t in range(sectors)]).astype(BF16)
    second_x = send(sent, over_x)

    held = jnp.stack([total(2 * y + k, 0) for k in range(2)]) + first_y.astype(F32)
    first_x = send(of_x(held, 1 - x).astype(BF16), over_x)
    second = jnp.stack([of_x(total(t, quarter), x) for t in range(sectors)])
    second = (second + second_x.astype(F32)).reshape(2, 2, depth, rows, quarter)
    second_y = send(jnp.where(y == 0, second[1], second[0]).astype(BF16), over_y)

    first = of_x(held, x) + first_x.astype(F32)
    second = jnp.where(y == 0, second[0], second[1]) + second_y.astype(F32)
    chip = jnp.concatenate([first, second], axis=-1)

    def at_z(index):
        return lax.dynamic_index_in_dim(chip, index % depth, 1, keepdims=False)

    mine = at_z(z)
    if depth <= 4:
        for shift in range(1, depth):
            away = at_z(z + shift).astype(BF16)
            mine = mine + send(
                away, lambda z, x, y, c: ((z + shift) % depth, x, y, c)
            ).astype(F32)
    else:
        groups = [[d * 2 + side for d in range(depth)] for side in range(2)]
        everyone = lax.all_to_all(
            chip.astype(BF16), "pair", 1, 1, tiled=True, axis_index_groups=groups
        )
        mine = jnp.sum(everyone.astype(F32), axis=1)

    swapped = send(jnp.where(c == 0, mine[1], mine[0]), over_core)
    staying = jnp.where(c == 0, mine[0], mine[1])
    sigma = jnp.concatenate(
        [jnp.where(c == 0, staying, swapped), jnp.where(c == 0, swapped, staying)], axis=1
    )
    return (sigma * (row_used[:, None] & used[None, :]).astype(F32))[None]


def solution(mesh):
    placed = (
        P("sector", "pair", None),
        P("pair", "sector", None, None),
        P("pair", "sector", None, None),
        P("pair", "sector"),
        P(),
        P("pair"),
        P(),
    )
    return jax.shard_map(
        body, mesh=mesh, in_specs=placed, out_specs=P("sector", "pair", None), check_vma=False
    )
```

```python
import jax
import jax.numpy as jnp
from jax import lax
from jax.sharding import PartitionSpec as P

AXES = ("pair", "sector")
F32 = jnp.float32
BF16 = jnp.bfloat16


def route(pairs, sectors, move, allowed=lambda z, x, y, c: True):
    links = []
    for p in range(pairs):
        for s in range(sectors):
            spot = (p // 2, p % 2, s // 2, s % 2)
            if not allowed(*spot):
                continue
            z, x, y, c = move(*spot)
            if 0 <= z < pairs // 2:
                links.append((p * sectors + s, (z * 2 + x) * sectors + y * 2 + c))
    return links


def body(wave, left_ops, right_ops, targets, sector_sizes, pair_ids, pair_coefficients):
    block = wave.shape[2]
    rows = wave.shape[1]
    slots = left_ops.shape[0]
    pairs = lax.axis_size("pair")
    sectors = lax.axis_size("sector")
    depth = pairs // 2
    half = block // 2
    chunks = 2
    wide = half // chunks
    part = wide // 2
    own_pair = lax.axis_index("pair")
    own_sector = lax.axis_index("sector")
    z, x = own_pair >> 1, own_pair & 1
    y, c = own_sector >> 1, own_sector & 1

    def send(value, move, allowed=lambda z, x, y, c: True):
        return lax.ppermute(value, AXES, route(pairs, sectors, move, allowed))

    def over_core(z, x, y, c):
        return z, x, y, 1 - c

    def over_x(z, x, y, c):
        return z, 1 - x, y, c

    def over_y(z, x, y, c):
        return z, x, 1 - y, c

    own_size = jnp.sum(jnp.where(jnp.arange(sectors) == own_sector, sector_sizes, 0))
    ids = jnp.arange(block, dtype=jnp.int32)
    used = ids < own_size
    row_used = own_pair * rows + jnp.arange(rows, dtype=jnp.int32) < own_size

    table_ids = jnp.arange(pair_coefficients.shape[0], dtype=jnp.int32)
    factor = jnp.sum(
        jnp.where(pair_ids[:, None] == table_ids[None, :], pair_coefficients[None, :], 0.0), axis=1
    )
    own_targets = targets[:, 0]
    other_targets = send(own_targets, over_core)

    own = wave[0]
    if depth <= 4:
        ups, downs = [], []
        up = down = own
        pieces = [(own, send(own, over_x))]
        for step in range(1, depth):
            up = send(up, lambda z, x, y, c: (z + 1, x, y, c), lambda z, x, y, c: z + 1 >= step)
            down = send(
                down, lambda z, x, y, c: (z - 1, x, y, c), lambda z, x, y, c: z - 1 < depth - step
            )
            ups.append((up, send(up, over_x, lambda z, x, y, c: z >= step)))
            downs.append((down, send(down, over_x, lambda z, x, y, c: z < depth - step)))
        chain = ups[::-1] + pieces + downs
        line = []
        for mine, theirs in chain:
            line.append(jnp.where(x == 0, mine, theirs))
            line.append(jnp.where(x == 0, theirs, mine))
        line = jnp.concatenate(line, axis=0)
        gathered = lax.dynamic_slice_in_dim(line, (depth - 1 - z) * 2 * rows, block, axis=0)
    else:
        gathered = lax.all_gather(own, "pair", axis=0, tiled=True)
    masked = gathered * (used[:, None] & used[None, :]).astype(gathered.dtype)

    lefts = [
        jnp.dot(left_ops[slot, 0], masked, preferred_element_type=F32).astype(BF16)
        for slot in range(slots)
    ]

    aims = jnp.concatenate([own_targets, other_targets])
    order = jnp.arange(sectors, dtype=jnp.int32) ^ (2 * y)
    near = (aims[:, None] == order[None, :]).astype(F32)
    every = (aims[:, None] == jnp.arange(sectors, dtype=jnp.int32)[None, :]).astype(F32)
    near, every, factor = lax.optimization_barrier((near, every, factor))

    def terms_of(core, chunk, lefts):
        start = core * half + chunk * wide
        terms = []
        for slot in range(slots):
            mat = lax.dynamic_slice_in_dim(right_ops[slot, 0], start, wide, axis=0)
            term = lax.dot_general(
                lefts[slot], mat, (((1,), (1,)), ((), ())), preferred_element_type=F32
            )
            terms.append(term * factor[slot])
        return terms

    def of_x(value, side):
        return jnp.where(side == 0, value[..., 0, :, :], value[..., 1, :, :])

    marks = {}

    def after(phase, values):
        if phase in marks:
            values, _ = lax.optimization_barrier((values, marks[phase]))
        return values

    def scatter(chunk):
        left = after(0, lefts)
        given = jnp.stack([t.astype(BF16) for t in terms_of(1 - c, chunk, left)])
        marks[0] = given
        taken = send(given, over_core)
        kept = terms_of(c, chunk, left)
        kept, taken = after(1, (kept, taken))
        terms = kept + [taken[slot].astype(F32) for slot in range(slots)]

        def total(weights, first):
            result = 0.0
            for i, term in enumerate(terms):
                result = result + weights[i][:, None, None] * term[None, :, first : first + part]
            return result.reshape(weights.shape[1], depth, 2, rows, part)

        to_y = total(near[:, 2:], 0).astype(BF16)
        to_x = of_x(total(every, part), 1 - x).astype(BF16)
        marks[1] = (to_y, to_x)
        first_y, second_x = send(to_y, over_y), send(to_x, over_x)
        first_y, second_x = after(2, (first_y, second_x))
        held = total(near[:, :2], 0) + first_y.astype(F32)
        to_x = of_x(held, 1 - x).astype(BF16)
        second = of_x(total(every, part), x) + second_x.astype(F32)
        second = second.reshape(2, 2, depth, rows, part)
        to_y = jnp.where(y == 0, second[1], second[0]).astype(BF16)
        marks[2] = (to_x, to_y)
        first_x, second_y = send(to_x, over_x), send(to_y, over_y)
        first = of_x(held, x) + first_x.astype(F32)
        second = jnp.where(y == 0, second[0], second[1]) + second_y.astype(F32)
        chip = jnp.concatenate([first, second], axis=-1)

        def at_z(index):
            return lax.dynamic_index_in_dim(chip, lax.rem(index, depth), 1, keepdims=False)

        mine = at_z(z)
        if depth <= 4:
            for shift in range(1, depth):
                away = at_z(z + shift).astype(BF16)
                mine = mine + send(
                    away, lambda z, x, y, c: ((z + shift) % depth, x, y, c)
                ).astype(F32)
        else:
            groups = [[d * 2 + side for d in range(depth)] for side in range(2)]
            everyone = lax.all_to_all(
                chip.astype(BF16), "pair", 1, 1, tiled=True, axis_index_groups=groups
            )
            mine = jnp.sum(everyone.astype(F32), axis=1)
        return mine

    mine = jnp.concatenate([scatter(chunk) for chunk in range(chunks)], axis=-1)

    swapped = send(jnp.where(c == 0, mine[1], mine[0]), over_core)
    staying = jnp.where(c == 0, mine[0], mine[1])
    sigma = jnp.concatenate(
        [jnp.where(c == 0, staying, swapped), jnp.where(c == 0, swapped, staying)], axis=1
    )
    return (sigma * (row_used[:, None] & used[None, :]).astype(F32))[None]


def solution(mesh):
    placed = (
        P("sector", "pair", None),
        P("pair", "sector", None, None),
        P("pair", "sector", None, None),
        P("pair", "sector"),
        P(),
        P("pair"),
        P(),
    )
    return jax.shard_map(
        body, mesh=mesh, in_specs=placed, out_specs=P("sector", "pair", None), check_vma=False
    )
```

```python
import jax
import jax.numpy as jnp
from jax import lax
from jax.sharding import PartitionSpec as P

AXES = ("pair", "sector")
F32 = jnp.float32
BF16 = jnp.bfloat16


def route(pairs, sectors, move, allowed=lambda z, x, y, c: True):
    links = []
    for p in range(pairs):
        for s in range(sectors):
            spot = (p // 2, p % 2, s // 2, s % 2)
            if not allowed(*spot):
                continue
            z, x, y, c = move(*spot)
            if 0 <= z < pairs // 2:
                links.append((p * sectors + s, (z * 2 + x) * sectors + y * 2 + c))
    return links


def body(wave, left_ops, right_ops, targets, sector_sizes, pair_ids, pair_coefficients):
    block = wave.shape[2]
    rows = wave.shape[1]
    slots = left_ops.shape[0]
    pairs = lax.axis_size("pair")
    sectors = lax.axis_size("sector")
    depth = pairs // 2
    half = block // 2
    chunks = 2
    wide = half // chunks
    part = wide // 2
    own_pair = lax.axis_index("pair")
    own_sector = lax.axis_index("sector")
    z, x = own_pair >> 1, own_pair & 1
    y, c = own_sector >> 1, own_sector & 1

    def send(value, move, allowed=lambda z, x, y, c: True):
        return lax.ppermute(value, AXES, route(pairs, sectors, move, allowed))

    def over_core(z, x, y, c):
        return z, x, y, 1 - c

    def over_x(z, x, y, c):
        return z, 1 - x, y, c

    def over_y(z, x, y, c):
        return z, x, 1 - y, c

    own_size = jnp.sum(jnp.where(jnp.arange(sectors) == own_sector, sector_sizes, 0))
    ids = jnp.arange(block, dtype=jnp.int32)
    used = ids < own_size
    row_used = own_pair * rows + jnp.arange(rows, dtype=jnp.int32) < own_size

    table_ids = jnp.arange(pair_coefficients.shape[0], dtype=jnp.int32)
    factor = jnp.sum(
        jnp.where(pair_ids[:, None] == table_ids[None, :], pair_coefficients[None, :], 0.0), axis=1
    )
    own_targets = targets[:, 0]
    other_targets = send(own_targets, over_core)

    own = wave[0]
    if depth <= 4:
        shifts = sorted(range(1, depth), key=lambda k: -min(k, depth - k))
        behind = {0: own}
        for k in shifts:
            behind[k] = send(own, lambda z, x, y, c: ((z + k) % depth, x, y, c))
        across = {k: send(behind[k], over_x) for k in [0] + shifts}
        chain = [(behind[k % depth], across[k % depth]) for k in range(depth - 1, -depth, -1)]
        line = []
        for mine, theirs in chain:
            line.append(jnp.where(x == 0, mine, theirs))
            line.append(jnp.where(x == 0, theirs, mine))
        line = jnp.concatenate(line, axis=0)
        gathered = lax.dynamic_slice_in_dim(line, (depth - 1 - z) * 2 * rows, block, axis=0)
    else:
        gathered = lax.all_gather(own, "pair", axis=0, tiled=True)
    masked = gathered * (used[:, None] & used[None, :]).astype(gathered.dtype)

    lefts = [
        jnp.dot(left_ops[slot, 0], masked, preferred_element_type=F32).astype(BF16)
        for slot in range(slots)
    ]

    aims = jnp.concatenate([own_targets, other_targets])
    order = jnp.arange(sectors, dtype=jnp.int32) ^ (2 * y)
    near = (aims[:, None] == order[None, :]).astype(F32)
    every = (aims[:, None] == jnp.arange(sectors, dtype=jnp.int32)[None, :]).astype(F32)
    near, every, factor = lax.optimization_barrier((near, every, factor))

    def terms_of(core, chunk, lefts):
        start = core * half + chunk * wide
        terms = []
        for slot in range(slots):
            mat = lax.dynamic_slice_in_dim(right_ops[slot, 0], start, wide, axis=0)
            term = lax.dot_general(
                lefts[slot], mat, (((1,), (1,)), ((), ())), preferred_element_type=F32
            )
            terms.append(term * factor[slot])
        return terms

    def of_x(value, side):
        return jnp.where(side == 0, value[..., 0, :, :], value[..., 1, :, :])

    marks = {}

    def after(phase, values):
        if phase in marks:
            values, _ = lax.optimization_barrier((values, marks[phase]))
        return values

    def scatter(chunk):
        left = after(0, lefts)
        given = jnp.stack([t.astype(BF16) for t in terms_of(1 - c, chunk, left)])
        marks[0] = given
        taken = send(given, over_core)
        kept = terms_of(c, chunk, left)
        kept, taken = after(1, (kept, taken))
        terms = kept + [taken[slot].astype(F32) for slot in range(slots)]

        def total(weights, first):
            result = 0.0
            for i, term in enumerate(terms):
                result = result + weights[i][:, None, None] * term[None, :, first : first + part]
            return result.reshape(weights.shape[1], depth, 2, rows, part)

        to_y = total(near[:, 2:], 0).astype(BF16)
        to_x = of_x(total(every, part), 1 - x).astype(BF16)
        marks[1] = (to_y, to_x)
        first_y, second_x = send(to_y, over_y), send(to_x, over_x)
        first_y, second_x = after(2, (first_y, second_x))
        held = total(near[:, :2], 0) + first_y.astype(F32)
        to_x = of_x(held, 1 - x).astype(BF16)
        second = of_x(total(every, part), x) + second_x.astype(F32)
        second = second.reshape(2, 2, depth, rows, part)
        to_y = jnp.where(y == 0, second[1], second[0]).astype(BF16)
        marks[2] = (to_x, to_y)
        first_x, second_y = send(to_x, over_x), send(to_y, over_y)
        first = of_x(held, x) + first_x.astype(F32)
        second = jnp.where(y == 0, second[0], second[1]) + second_y.astype(F32)
        chip = jnp.concatenate([first, second], axis=-1)

        def at_z(index):
            return lax.dynamic_index_in_dim(chip, lax.rem(index, depth), 1, keepdims=False)

        mine = at_z(z)
        if depth <= 4:
            for shift in range(1, depth):
                away = at_z(z + shift).astype(BF16)
                mine = mine + send(
                    away, lambda z, x, y, c: ((z + shift) % depth, x, y, c)
                ).astype(F32)
        else:
            groups = [[d * 2 + side for d in range(depth)] for side in range(2)]
            everyone = lax.all_to_all(
                chip.astype(BF16), "pair", 1, 1, tiled=True, axis_index_groups=groups
            )
            mine = jnp.sum(everyone.astype(F32), axis=1)
        return mine

    mine = jnp.concatenate([scatter(chunk) for chunk in range(chunks)], axis=-1)

    swapped = send(jnp.where(c == 0, mine[1], mine[0]), over_core)
    staying = jnp.where(c == 0, mine[0], mine[1])
    sigma = jnp.concatenate(
        [jnp.where(c == 0, staying, swapped), jnp.where(c == 0, swapped, staying)], axis=1
    )
    return (sigma * (row_used[:, None] & used[None, :]).astype(F32))[None]


def solution(mesh):
    placed = (
        P("sector", "pair", None),
        P("pair", "sector", None, None),
        P("pair", "sector", None, None),
        P("pair", "sector"),
        P(),
        P("pair"),
        P(),
    )
    return jax.shard_map(
        body, mesh=mesh, in_specs=placed, out_specs=P("sector", "pair", None), check_vma=False
    )
```
